128 devices in a mesh: local: 2 (over core), data: 64 (over z, y, x).
Axes of the slice: x: 4, y: 4, z: 4, core: 2. Of those that a mesh axis runs over, the one named last changes fastest.
Arguments:
- tokens: bfloat16 [65536, 1024], P(('data', 'local'))
- cotangent: bfloat16 [65536, 1024], P(('data', 'local'))
- w_up: bfloat16 [4, 1024, 4096], P(None, ('data', 'local'))
- w_down: bfloat16 [4, 4096, 1024], P(None, ('data', 'local'))
- lora_a: float32 [4, 1024, 8], replicated
- lora_b: float32 [4, 8, 4096], replicated
Outputs:
- output 1: bfloat16 [65536, 1024], P(('data', 'local'))
- output 2: bfloat16 [65536, 1024], P(('data', 'local'))
- output 3: float32 [4, 1024, 8], replicated
- output 4: float32 [4, 8, 4096], replicated
All inputs are finite; a program needn't handle non-finite values.
Results may differ from the reference program's by a relative error of at most 0.0188455.
Values are sent between devices in bfloat16 or wider.
A program may use at most 1 GiB of HBM per device.

```python
import jax
import jax.numpy as jnp
from jax import lax

TOKENS = 512
NUM_DEVICES = 128
HIDDEN = 1024
FF_DIM = 4096
RANK = 8
LAYERS = 4

TOTAL_TOKENS = NUM_DEVICES * TOKENS


def setup_inputs(seed: int = 0) -> dict:
    keys = jax.random.split(jax.random.key(seed), 6)
    tokens = jax.random.normal(keys[0], (TOTAL_TOKENS, HIDDEN), jnp.float32).astype(jnp.bfloat16)
    cotangent = jax.random.normal(keys[1], (TOTAL_TOKENS, HIDDEN), jnp.float32).astype(jnp.bfloat16)
    w_up = (jax.random.normal(keys[2], (LAYERS, HIDDEN, FF_DIM), jnp.float32) * HIDDEN ** -0.5).astype(jnp.bfloat16)
    w_down = (jax.random.normal(keys[3], (LAYERS, FF_DIM, HIDDEN), jnp.float32) * FF_DIM ** -0.5).astype(jnp.bfloat16)
    lora_a = jax.random.normal(keys[4], (LAYERS, HIDDEN, RANK), jnp.float32) * HIDDEN ** -0.5
    lora_b = jax.random.normal(keys[5], (LAYERS, RANK, FF_DIM), jnp.float32) * (0.5 / RANK) ** 0.5
    return {"tokens": tokens, "cotangent": cotangent, "w_up": w_up, "w_down": w_down, "lora_a": lora_a, "lora_b": lora_b}


def layer_forward(resid, w_in, w_out, adapt_a, adapt_b):
    resid_f = resid.astype(jnp.float32)
    inv_rms = lax.rsqrt(jnp.mean(resid_f * resid_f, axis=-1, keepdims=True) + 1e-6)
    normed = (resid_f * inv_rms).astype(jnp.bfloat16)
    low_rank = jnp.dot(normed.astype(jnp.float32), adapt_a)
    pre_act = (jnp.dot(normed, w_in, preferred_element_type=jnp.float32) + jnp.dot(low_rank, adapt_b)).astype(jnp.bfloat16)
    hidden_act = jax.nn.gelu(pre_act.astype(jnp.float32), approximate=True).astype(jnp.bfloat16)
    return (resid_f + jnp.dot(hidden_act, w_out, preferred_element_type=jnp.float32)).astype(jnp.bfloat16)


def stack_forward(resid, w_up, w_down, lora_a, lora_b):
    def body(carry, weights):
        w_in, w_out, adapt_a, adapt_b = weights
        return layer_forward(carry, w_in, w_out, adapt_a, adapt_b), None
    result, _ = lax.scan(body, resid, (w_up, w_down, lora_a, lora_b))
    return result


def reference(tokens, cotangent, w_up, w_down, lora_a, lora_b):
    tok_blocks = tokens.reshape(NUM_DEVICES, TOKENS, HIDDEN)
    cot_blocks = cotangent.reshape(NUM_DEVICES, TOKENS, HIDDEN)

    def block_step(running, pair):
        blk_tokens, blk_cot = pair
        result, pullback = jax.vjp(lambda blk_in, adapt_a, adapt_b: stack_forward(blk_in, w_up, w_down, adapt_a, adapt_b), blk_tokens, lora_a, lora_b)
        grad_x, grad_a, grad_b = pullback(blk_cot)
        return (running[0] + grad_a, running[1] + grad_b), (result, grad_x)

    start_sums = (jnp.zeros(lora_a.shape, jnp.float32), jnp.zeros(lora_b.shape, jnp.float32))
    (sum_a, sum_b), (out_blocks, grad_blocks) = lax.scan(block_step, start_sums, (tok_blocks, cot_blocks))
    return (out_blocks.reshape(TOTAL_TOKENS, HIDDEN), grad_blocks.reshape(TOTAL_TOKENS, HIDDEN), sum_a, sum_b)
```

```python
import jax
import jax.numpy as jnp
from jax import lax
from jax.experimental import pallas as pl
from jax.experimental.pallas import tpu as pltpu
from jax.sharding import PartitionSpec as P

GROUP = ("data", "local")
EPS = 1e-6
MESH_ID = pl.DeviceIdType.MESH
F32 = jnp.float32
BF16 = jnp.bfloat16
H = 1024
FH = 2048
NT = 1024
GT = 256
LAYERS = RING = 4
CR = 256
UNIT = 512
LANE = 128
SUB = 8
RB = 128
QW = 768
GROUPS = ((0, 2), (2, 2))
COLS_UP = ((0, 640), (640, 640), (1280, 768))
COLS_DOWN = ((0, 384), (384, 384), (768, 256))
GELU_K = 0.7978845608028654
GELU_C = 0.044715


def split3(val):
    hi = val.astype(BF16).astype(F32)
    rest = val - hi
    mid = rest.astype(BF16).astype(F32)
    return hi, mid, (rest - mid).astype(BF16).astype(F32)


def gelu(pre):
    sq = pre * pre
    t = jnp.tanh(pre * (GELU_K + (GELU_K * GELU_C) * sq))
    return pre * (0.5 * t + 0.5)


def gelu_grad(pre):
    sq = pre * pre
    t = jnp.tanh(pre * (GELU_K + (GELU_K * GELU_C) * sq))
    slope = 0.5 * GELU_K + (1.5 * GELU_K * GELU_C) * sq
    return (0.5 * t + 0.5) + pre * ((1.0 - t * t) * slope)


def lane_sum3(rep):
    return rep + pltpu.roll(rep, 120, 1) + pltpu.roll(rep, 112, 1)


def spread(val):
    hi, mid, lo = split3(val)
    lane = lax.broadcasted_iota(jnp.int32, val.shape, 1)
    out = jnp.where(lane < 24, hi, jnp.where(lane < 48, mid, jnp.where(lane < 72, lo, 0.0)))
    return out.astype(BF16)


def span(i, n):
    return pl.ds(pl.multiple_of(i * n, n), n)


def ring(c, delta):
    return lax.rem(c + delta, RING)


def parts_sum(g):
    return g[0:SUB] + g[24:32] + g[48:56]


def dot(a, b):
    return lax.dot_general(a, b, (((1,), (0,)), ((), ())), preferred_element_type=F32)


def dot_nt(a, b):
    return lax.dot_general(a, b, (((1,), (1,)), ((), ())), preferred_element_type=F32)


def dot_tn(a, b):
    return lax.dot_general(a, b, (((0,), (0,)), ((), ())), preferred_element_type=F32)


def kernel(tok, cot, up, down, arep, bhalf,
           out, gout, grads, presave,
           w1, w2, apat, bpat, stage_a, stage_b, ubuf, dbuf, sbuf, pre, ybuf, yrecv, dl, dlrecv, vbuf, xbuf,
           gpart, rz, ry, rx, rsum, rpart,
           lsem, xsem, gssem, grsem, ysend, yrecv_sem, usend, urecv, dsend, drecv, lsend, lrecv, psem, osem, assem, arsem, prsem):
    d = lax.axis_index("data")
    j = lax.axis_index("local")
    oth = 1 - j
    y = d // RING
    z, y, x = y // RING, ring(y, 0), ring(d, 0)
    me = (z, y, x)

    def data_id(dim, delta):
        c = list(me)
        c[dim] = ring(c[dim], delta + RING)
        return {"data": (c[0] * RING + c[1]) * RING + c[2]}

    partner = {"local": oth}

    def remote(src, dst, ss, rs, dev):
        return pltpu.make_async_remote_copy(src_ref=src, dst_ref=dst, send_sem=ss, recv_sem=rs, device_id=dev, device_id_type=MESH_ID)

    def block(p, k, v, l0, nl, mat):
        dims = [None] * 3
        for i in range(3):
            q = (p + i) % 3
            dims[q] = slice(None) if i < k else (v if i == k else me[q])
        c0, cn = (COLS_UP if mat == 0 else COLS_DOWN)[p]
        return (w1, w2)[mat].at[pl.ds(l0, nl), dims[0], dims[1], dims[2], :, pl.ds(c0, cn)]

    def hop(p, k, v, g, l0, nl, mat, msg, delta):
        r = block(p, k, v, l0, nl, mat)
        return remote(r, r, gssem.at[mat, k], grsem.at[p, k, msg, g], data_id((p + k) % 3, delta))

    def full(k, g, l0, nl):
        for p in range(3):
            c = me[(p + k) % 3]
            hop(p, k, c, g, l0, nl, 0, 0, 1).start()
            hop(p, k, c, g, l0, nl, 1, 3, -1).start()
            hop(p, k, c, g, l0, nl, 0, 1, -1).start()
            hop(p, k, c, g, l0, nl, 1, 2, 1).start()

    def forward_half(k, g, l0, nl):
        for p in range(3):
            c = me[(p + k) % 3]
            left, right = ring(c, 3), ring(c, 1)
            hop(p, k, left, g, l0, nl, 0, 0, 1).wait_recv()
            hop(p, k, left, g, l0, nl, 0, 4, 1).start()
            hop(p, k, right, g, l0, nl, 1, 3, -1).wait_recv()
            hop(p, k, right, g, l0, nl, 1, 5, -1).start()

    def arrive(k, g, l0, nl):
        for p in range(3):
            c = me[(p + k) % 3]
            left, right, opp = ring(c, 3), ring(c, 1), ring(c, 2)
            hop(p, k, right, g, l0, nl, 0, 1, -1).wait_recv()
            hop(p, k, left, g, l0, nl, 1, 2, 1).wait_recv()
            hop(p, k, opp, g, l0, nl, 0, 4, 1).wait_recv()
            hop(p, k, opp, g, l0, nl, 1, 5, -1).wait_recv()

    def drain_gather():
        for mat, ref in ((0, w1), (1, w2)):
            for k, r in ((0, ref.at[:, 0, 0, 0:3]), (1, ref.at[:, 0, 0:3]), (2, ref.at[:, 0:3])):
                remote(r, r, gssem.at[mat, k], grsem.at[0, 0, 0, 0], data_id(0, 1)).wait_send()

    loads = [
        pltpu.make_async_copy(up.at[j], w1.at[:, z, y, x, span(j, SUB)], lsem.at[0]),
        pltpu.make_async_copy(down, w2.at[:, z, y, x], lsem.at[1]),
        pltpu.make_async_copy(tok, xbuf.at[0], lsem.at[2]),
        pltpu.make_async_copy(cot, dbuf.at[:, j], lsem.at[3]),
        pltpu.make_async_copy(arep, stage_a, lsem.at[4]),
        pltpu.make_async_copy(bhalf.at[j], stage_b, lsem.at[5]),
    ]
    for c in loads:
        c.start()
    bar = pltpu.get_barrier_semaphore()
    for dim in range(3):
        for delta in (1, 2, 3):
            pl.semaphore_signal(bar, inc=1, device_id=data_id(dim, delta), device_id_type=MESH_ID)
    pl.semaphore_signal(bar, inc=1, device_id=partner, device_id_type=MESH_ID)
    pl.semaphore_wait(bar, 10)

    mine_rows = w1.at[:, z, y, x, span(j, SUB)]
    other_rows = w1.at[:, z, y, x, span(oth, SUB)]
    ex_up = remote(up.at[oth], mine_rows, xsem.at[0], xsem.at[1], partner)
    ex_up.start()
    loads[0].wait()
    loads[1].wait()
    remote(up.at[oth], other_rows, xsem.at[0], xsem.at[1], partner).wait_recv()
    for g, (l0, nl) in enumerate(GROUPS):
        full(0, g, l0, nl)
    ex_cot = remote(cot, dbuf.at[:, j], xsem.at[2], xsem.at[3], partner)
    ex_cot.start()

    def inv_rms(xf):
        return lax.rsqrt(jnp.mean(xf * xf, axis=-1, keepdims=True) + EPS)

    def u_copy(c):
        return remote(ubuf.at[c, j], ubuf.at[c, j], usend.at[c], urecv.at[c], partner)

    def u_arrival(c):
        return remote(ubuf.at[c, oth], ubuf.at[c, oth], usend.at[c], urecv.at[c], partner)

    def y_copy(c):
        return remote(ybuf.at[oth], yrecv.at[c], ysend.at[0], yrecv_sem.at[c], partner)

    def l_copy(c):
        return remote(dl.at[oth], dlrecv.at[c], lsend.at[0], lrecv.at[c], partner)

    def d_copy(c):
        return remote(dbuf.at[c, j], dbuf.at[c, j], dsend.at[c], drecv.at[c], partner)

    def d_arrival(c):
        return remote(dbuf.at[c, oth], dbuf.at[c, oth], dsend.at[c], drecv.at[c], partner)

    def out_copy(c):
        return pltpu.make_async_copy(ubuf.at[c, j], out.at[c], osem.at[c])

    def gout_copy(c):
        return pltpu.make_async_copy(dbuf.at[c, j], gout.at[c], osem.at[2 + c])

    def send_u(l, c):
        @pl.loop(0, CR // RB)
        def _(i):
            rows = span(i, RB)
            xf = xbuf[l, c, rows].astype(F32)
            ubuf[c, j, rows] = (xf * inv_rms(xf)).astype(BF16)
        u_copy(c).start()

    loads[2].wait()
    for c in (0, 1):
        send_u(0, c)
    for g, (l0, nl) in enumerate(GROUPS):
        forward_half(0, g, l0, nl)

    loads[4].wait()
    loads[5].wait()

    @pl.loop(0, LAYERS * SUB)
    def _(i):
        l, r = i // SUB, span(lax.rem(i, SUB), LANE)
        hi, mid, lo = split3(stage_a[l, r])
        group = lax.rem(lax.broadcasted_iota(jnp.int32, (LANE, LANE), 1) // SUB, 3)
        apat[l, r] = jnp.where(group == 0, hi, jnp.where(group == 1, mid, lo)).astype(BF16)

    @pl.loop(0, LAYERS * SUB)
    def _(i):
        l, r = i // SUB, span(lax.rem(i, SUB), CR)
        parts = split3(stage_b[l, :, r])
        bpat[l, :, r] = jnp.concatenate([parts[m % 3] for m in range(16)], axis=0).astype(BF16)

    for g, (l0, nl) in enumerate(GROUPS):
        arrive(0, g, l0, nl)
        full(1, g, l0, nl)
    for g, (l0, nl) in enumerate(GROUPS):
        forward_half(1, g, l0, nl)
    arrive(1, 0, 0, 2)
    full(2, 0, 0, 1)
    full(2, 1, 1, 1)
    arrive(1, 1, 2, 2)
    forward_half(2, 0, 0, 1)
    full(2, 2, 2, 1)

    def ncol(n):
        return span(n, NT)

    def w1_tile(l, n):
        return w1[l, :, :, :, :, ncol(n)].reshape(H, NT)

    def w2_tile(l, n):
        return w2[l, :, :, :, :, ncol(n)].reshape(FH, NT)

    def pre_save(l, c):
        return pltpu.make_async_copy(pre.at[c], presave.at[l, c], psem.at[c])

    def pre_load(l, c):
        return pltpu.make_async_copy(presave.at[l, c], pre.at[c], psem.at[c])

    def up_phase(l, c):
        u = ubuf[c].reshape(UNIT, H)
        vsplit = spread(lane_sum3(dot(u, apat[l])))
        vbuf[l, c] = vsplit

        @pl.when(l > 0)
        def _():
            pre_save(l - 1, c).wait()

        @pl.loop(0, FH // NT)
        def _(n):
            acc = dot(ubuf[c].reshape(UNIT, H), w1_tile(l, n)) + dot(vbuf[l, c], bpat[l, :, ncol(n)])
            a = acc.astype(BF16)
            pre[c, :, ncol(n)] = a
            sbuf[:, ncol(n)] = gelu(a.astype(F32)).astype(BF16)

        @pl.when(l < LAYERS - 1)
        def _():
            pre_save(l, c).start()

    def down_phase(l, c):
        @pl.loop(0, H // NT)
        def _(n):
            ybuf[:, :, ncol(n)] = dot(sbuf[...], w2_tile(l, n)).reshape(2, CR, NT)
        y_copy(c).start()

    def finish(l, c):
        y_copy(c).wait_recv()
        u_copy(c).wait_send()

        @pl.loop(0, CR // RB)
        def _(i):
            rows = span(i, RB)
            new = (xbuf[l, c, rows].astype(F32) + (ybuf[j, rows] + yrecv[c, rows])).astype(BF16)

            @pl.when(l < LAYERS - 1)
            def _():
                xbuf[l + 1, c, rows] = new
                xf = new.astype(F32)
                ubuf[c, j, rows] = (xf * inv_rms(xf)).astype(BF16)

            @pl.when(l == LAYERS - 1)
            def _():
                ubuf[c, j, rows] = new

        @pl.when(l < LAYERS - 1)
        def _():
            u_copy(c).start()

        @pl.when(l == LAYERS - 1)
        def _():
            out_copy(c).start()

    @pl.loop(0, LAYERS)
    def _(l):
        @pl.when(l + 1 < LAYERS)
        def _():
            forward_half(2, l + 1, l + 1, 1)

        @pl.when(l + 3 < LAYERS)
        def _():
            full(2, l + 3, l + 3, 1)

        arrive(2, l, l, 1)
        u_arrival(0).wait_recv()
        up_phase(l, 0)

        @pl.when(l > 0)
        def _():
            finish(l - 1, 1)
            y_copy(1).wait_send()

        down_phase(l, 0)
        u_arrival(1).wait_recv()
        up_phase(l, 1)
        finish(l, 0)
        y_copy(0).wait_send()
        down_phase(l, 1)

    def dpre_phase(l, c):
        @pl.when(l < LAYERS - 1)
        def _():
            pre_load(l, c).wait()

        @pl.loop(0, FH // NT)
        def _(n):
            w = w2[l, span(n, NT // UNIT)].reshape(NT, H)
            dh = dot_nt(dbuf[c].reshape(UNIT, H), w).astype(BF16).astype(F32)
            a = pre[c, :, ncol(n)].astype(F32)
            sbuf[:, ncol(n)] = (gelu_grad(a) * dh).astype(BF16)

        @pl.when(l > 0)
        def _():
            pre_load(l - 1, c).start()

    def low_phase(l, c):
        dl[...] = lane_sum3(dot_nt(sbuf[...], bpat[l])).reshape(2, CR, LANE)
        l_copy(c).start()
        for t in range(FH // GT):
            g = parts_sum(dot_tn(vbuf[l, c], sbuf[:, pl.ds(t * GT, GT)]))
            dst = (l, t // 3, slice(None), pl.ds((t % 3) * GT, GT))
            gpart[dst] = gpart[dst] + g if c else g

    def dmain_phase(l, c):
        @pl.loop(0, H // NT)
        def _(n):
            w = w1[l, span(n, NT // CR)].reshape(NT, FH)
            ybuf[:, :, ncol(n)] = dot_nt(sbuf[...], w).reshape(2, CR, NT)
        y_copy(c).start()

    def back_finish(l, c):
        l_copy(c).wait_recv()
        y_copy(c).wait_recv()
        dlow = dl[j] + dlrecv[c]
        dsplit = spread(dlow)

        @pl.when(l < LAYERS - 1)
        def _():
            d_copy(c).wait_send()

        @pl.when(l == LAYERS - 1)
        def _():
            out_copy(c).wait()

        @pl.loop(0, CR // RB)
        def _(i):
            rows = span(i, RB)
            xf = xbuf[l, c, rows].astype(F32)
            inv = inv_rms(xf)
            ubuf[c, j, rows] = (xf * inv).astype(BF16)
            dl[j, rows] = dl[j, rows] + dlrecv[c, rows]
            dside = dot_nt(spread(dl[j, rows]), apat[l]).astype(BF16).astype(F32)
            dmain = (ybuf[j, rows] + yrecv[c, rows]).astype(BF16).astype(F32)
            dn = (dmain + dside).astype(BF16).astype(F32)
            rowdot = jnp.mean(xf * dn, axis=-1, keepdims=True)
            dx = dbuf[c, j, rows].astype(F32) + inv * dn - xf * (inv * inv * inv) * rowdot
            dbuf[c, j, rows] = dx.astype(BF16)

        @pl.when(l > 0)
        def _():
            d_copy(c).start()

        @pl.when(l == 0)
        def _():
            gout_copy(c).start()

        for t in range(H // GT):
            g = parts_sum(dot_tn(dsplit, ubuf[c, j, :, pl.ds(t * GT, GT)]))
            tt = t + FH // GT
            dst = (l, tt // 3, slice(None), pl.ds((tt % 3) * GT, GT))
            gpart[dst] = gpart[dst] + g if c else g

    def line_copies(l, stage, dim, src, dst_buf):
        return [remote(src(ring(me[dim], k)), dst_buf.at[l, me[dim]], assem.at[stage, l, k - 1], arsem.at[stage, l, k - 1], data_id(dim, k)) for k in (1, 2, 3)]

    def line_wait(l, stage, dim, buf):
        for k in (1, 2, 3):
            v = ring(me[dim], RING - k)
            remote(buf.at[l, v], buf.at[l, v], assem.at[stage, l, k - 1], arsem.at[stage, l, k - 1], data_id(dim, k)).wait_recv()

    def sum4(buf, l):
        return (buf[l, 0] + buf[l, 1]) + (buf[l, 2] + buf[l, 3])

    def reduce_stage(l, s):
        if s == 0:
            for cp in line_copies(l, 0, 0, lambda q: gpart.at[l, q], rz):
                cp.start()
            rz[l, z] = gpart[l, z]
        elif s == 1:
            line_wait(l, 0, 0, rz)
            ry[l, y] = sum4(rz, l)
            for cp in line_copies(l, 1, 1, lambda q: ry.at[l, y], ry):
                cp.start()
        elif s == 2:
            line_wait(l, 1, 1, ry)
            rx[l, x] = sum4(ry, l)
            for cp in line_copies(l, 2, 2, lambda q: rx.at[l, x], rx):
                cp.start()
        elif s == 3:
            line_wait(l, 2, 2, rx)
            rsum[l, z] = sum4(rx, l)
            for cp in line_copies(l, 3, 0, lambda q: rsum.at[l, z], rsum):
                cp.start()
        elif s == 4:
            line_wait(l, 3, 0, rsum)
            remote(rsum.at[l], rpart.at[l], prsem.at[0, l], prsem.at[1, l], partner).start()
            pltpu.make_async_copy(rsum.at[l], grads.at[j, l], prsem.at[2, l]).start()
        else:
            remote(rsum.at[l], rpart.at[l], prsem.at[0, l], prsem.at[1, l], partner).wait_recv()
            pltpu.make_async_copy(rpart.at[l], grads.at[oth, l], prsem.at[3, l]).start()

    ex_cot_in = remote(cot, dbuf.at[:, oth], xsem.at[2], xsem.at[3], partner)
    loads[3].wait()
    ex_cot_in.wait_recv()
    ex_cot.wait_send()
    ex_up.wait_send()

    def back_layer(l, last):
        not_top = l < LAYERS - 1

        @pl.when(not_top)
        def _():
            d_arrival(0).wait_recv()

        dpre_phase(l, 0)

        @pl.when(l == LAYERS - 1)
        def _():
            finish(LAYERS - 1, 1)

        @pl.when(not_top)
        def _():
            back_finish(l + 1, 1)
            l_copy(1).wait_send()
            reduce_stage(l + 1, 0)

        y_copy(1).wait_send()
        low_phase(l, 0)
        dmain_phase(l, 0)

        @pl.when(not_top)
        def _():
            reduce_stage(l + 1, 1)
            d_arrival(1).wait_recv()

        dpre_phase(l, 1)

        @pl.when(not_top)
        def _():
            reduce_stage(l + 1, 2)

        back_finish(l, 0)
        l_copy(0).wait_send()
        y_copy(0).wait_send()
        low_phase(l, 1)

        @pl.when(not_top)
        def _():
            reduce_stage(l + 1, 3)

        dmain_phase(l, 1)

        @pl.when(not_top)
        def _():
            reduce_stage(l + 1, 4)
            reduce_stage(l + 1, 5)

    @pl.loop(0, LAYERS)
    def _(i):
        back_layer(LAYERS - 1 - i, False)

    back_finish(0, 1)
    for s in range(6):
        reduce_stage(0, s)
    l_copy(1).wait_send()
    y_copy(1).wait_send()
    for c in (0, 1):
        gout_copy(c).wait()

    @pl.loop(0, LAYERS)
    def _(l):
        for s in range(4):
            for k in range(3):
                r = rz.at[l, 0]
                remote(r, r, assem.at[s, l, k], arsem.at[s, l, k], data_id(0, 1)).wait_send()
        remote(rsum.at[l], rpart.at[l], prsem.at[0, l], prsem.at[1, l], partner).wait_send()
        pltpu.make_async_copy(rsum.at[l], grads.at[j, l], prsem.at[2, l]).wait()
        pltpu.make_async_copy(rpart.at[l], grads.at[oth, l], prsem.at[3, l]).wait()

    drain_gather()


TWO = (2,)
PERM = (3, 0, 1, 2, 4)


def device_step(tokens, cotangent, up_shards, down_shards, lora_a, lora_b):
    up = jnp.transpose(up_shards.reshape(LAYERS, SUB, 64, 2, 32), PERM).reshape(2, LAYERS, SUB, FH)
    bhalf = jnp.transpose(lora_b.reshape(LAYERS, SUB, 64, 2, 32), PERM).reshape(2, LAYERS, SUB, FH)
    arep = jnp.tile(lora_a, (1, 1, 16))
    hbm = pl.BlockSpec(memory_space=pl.ANY)
    dma = pltpu.SemaphoreType.DMA
    out, gout, grads, _ = pl.pallas_call(
        kernel,
        out_shape=(
            jax.ShapeDtypeStruct((2, CR, H), BF16),
            jax.ShapeDtypeStruct((2, CR, H), BF16),
            jax.ShapeDtypeStruct((2, LAYERS, 4, SUB, QW), F32),
            jax.ShapeDtypeStruct((LAYERS - 1, 2, UNIT, FH), BF16),
        ),
        in_specs=[hbm] * 6,
        out_specs=[hbm] * 4,
        scratch_shapes=[
            pltpu.VMEM((LAYERS, RING, RING, RING, 16, FH), BF16),
            pltpu.VMEM((LAYERS, RING, RING, RING, 32, H), BF16),
            pltpu.VMEM((LAYERS, H, LANE), BF16),
            pltpu.VMEM((LAYERS, LANE, FH), BF16),
            pltpu.VMEM((LAYERS, H, LANE), F32),
            pltpu.VMEM((LAYERS, SUB, FH), F32),
            pltpu.VMEM((2, 2, CR, H), BF16),
            pltpu.VMEM((2, 2, CR, H), BF16),
            pltpu.VMEM((UNIT, FH), BF16),
            pltpu.VMEM((2, UNIT, FH), BF16),
            pltpu.VMEM((2, CR, H), F32),
            pltpu.VMEM((2, CR, H), F32),
            pltpu.VMEM((2, CR, LANE), F32),
            pltpu.VMEM((2, CR, LANE), F32),
            pltpu.VMEM((LAYERS, 2, UNIT, LANE), BF16),
            pltpu.VMEM((LAYERS, 2, CR, H), BF16),
        ] + [pltpu.VMEM((LAYERS, 4, SUB, QW), F32)] * 6 + [
            dma((6,)), dma((LAYERS,)), dma((2, 3)), dma((3, 3, 6, LAYERS)),
            dma((1,)), dma(TWO), dma(TWO), dma(TWO), dma(TWO), dma(TWO), dma((1,)), dma(TWO),
            dma(TWO), dma((LAYERS,)), dma((LAYERS, LAYERS, 3)), dma((LAYERS, LAYERS, 3)), dma((LAYERS, LAYERS)),
        ],
        compiler_params=pltpu.CompilerParams(collective_id=0, has_side_effects=True, vmem_limit_bytes=67000000),
    )(tokens.reshape(2, CR, H), cotangent.reshape(2, CR, H), up, down_shards, arep, bhalf)
    g = jnp.transpose(grads, (0, 1, 3, 2, 4)).reshape(2, LAYERS, 8, 3072)
    grad_b = jnp.transpose(g[..., :FH].reshape(2, LAYERS, 8, 64, 32), (1, 2, 3, 0, 4)).reshape(LAYERS, 8, 4096)
    grad_a = jnp.transpose(g[0, :, :, FH:] + g[1, :, :, FH:], (0, 2, 1))
    return out.reshape(UNIT, H), gout.reshape(UNIT, H), grad_a, grad_b


def solution(mesh):
    tok_spec = P(GROUP, None)
    weight_spec = P(None, GROUP, None)
    return jax.shard_map(device_step, mesh=mesh, in_specs=(tok_spec, tok_spec, weight_spec, weight_spec, P(), P()),
                         out_specs=(tok_spec, tok_spec, P(), P()), check_vma=False)
```
